128 devices in a mesh: gx: 4 (over x_hi, core), gy: 32 (over x_lo, z, y).
Axes of the slice: x: 4 (x_hi: 2, x_lo: 2; x = x_hi * 2 + x_lo), y: 4, z: 4, core: 2. Of those that a mesh axis runs over, the one named last changes fastest.
Arguments:
- activations: bfloat16 [4096, 8192], P('gx', 'gy'), may hold values from -12 to 12
- out_grads: bfloat16 [4096, 16384], P('gx', 'gy'), may hold values from -12 to 12
- left_roots: float32 [128, 1024, 1024], P(('gx', 'gy')), may hold values from -20 to 20, as said below
- right_roots: float32 [128, 1024, 1024], P(('gx', 'gy')), may hold values from -20 to 20, as said below
Outputs:
- update: bfloat16 [8192, 16384], P(None, 'gy')
The draws below stay inside these ranges and needn't reach their ends.
Inputs may be any that keep to these rules, and one draw needn't show every extreme that they name: `left_roots`: each block is symmetric positive definite. `right_roots`: each block is symmetric positive definite.
All inputs are finite; a program needn't handle non-finite values.
Results may differ from the reference program's by a relative error of at most 0.001.
Values may be sent and summed in bfloat16 or wider, within the bound.
A program may use at most 128 MiB of HBM per device.

```python
import math
import jax
import jax.numpy as jnp
from jax import lax

D = 8192
BLK = 1024
TOKENS = 4096
COLS = 16384
NBLK = 128
N_GY = 32


def scaled_draw(key, row_count, width):
    key_scale, key_noise = jax.random.split(key, 2)
    feature_scale = jnp.exp(jax.random.uniform(key_scale, (width,), jnp.float32, math.log(0.3), math.log(3.0)))
    values = jax.random.normal(key_noise, (row_count, width), jnp.float32) * feature_scale[None, :]
    return jnp.clip(values, -12.0, 12.0).astype(jnp.bfloat16)


def draw_activations(key, part):
    return scaled_draw(jax.random.fold_in(key, 11), TOKENS, D)


def draw_out_grads(key, part):
    return scaled_draw(jax.random.fold_in(key, 23), TOKENS, COLS)


def root_draw(key, salt):
    base = jax.random.fold_in(key, salt)

    def single(index):
        sub = jax.random.fold_in(base, index)
        key_scale, key_noise = jax.random.split(sub)
        scales = jnp.exp(jax.random.uniform(key_scale, (BLK,), jnp.float32, math.log(0.3), math.log(3.0)))
        noise = jax.random.normal(key_noise, (BLK, BLK), jnp.float32)
        symmetric = (noise + noise.T) * (0.4 / math.sqrt(2.0 * BLK))
        core = jnp.eye(BLK, dtype=jnp.float32) + symmetric
        return scales[:, None] * core * scales[None, :]
    return lax.map(single, jnp.arange(NBLK, dtype=jnp.int32))


def draw_left_roots(key, part):
    return root_draw(key, 37)


def draw_right_roots(key, part):
    return root_draw(key, 41)


def setup_inputs(seed: int = 0) -> dict:
    splits = jax.random.split(jax.random.key(seed), 5)
    activations = draw_activations(jax.random.fold_in(splits[4], 71), 0)
    out_grads = draw_out_grads(jax.random.fold_in(splits[4], 71), 0)
    left_roots = draw_left_roots(jax.random.fold_in(splits[4], 71), 0)
    right_roots = draw_right_roots(jax.random.fold_in(splits[4], 71), 0)
    return dict(activations=activations, out_grads=out_grads, left_roots=left_roots, right_roots=right_roots)


epsilon = 1e-06

def precondition(items):
    grad_block, left_root, right_root = items
    shaped = jnp.dot(jnp.dot(left_root, grad_block, precision=lax.Precision.HIGHEST), right_root, precision=lax.Precision.HIGHEST)
    graft = jnp.sqrt(jnp.mean(grad_block * grad_block) + epsilon) / jnp.sqrt(jnp.mean(shaped * shaped) + epsilon)
    return (shaped * graft).astype(jnp.bfloat16)

def reference(activations, out_grads, left_roots, right_roots):
    weight_grad = lax.dot_general(activations, out_grads, (((0,), (0,)), ((), ())), preferred_element_type=jnp.float32)
    row_blocks = D // BLK
    col_blocks = COLS // BLK
    tiles = weight_grad.reshape(row_blocks, BLK, col_blocks, BLK).transpose(0, 2, 1, 3)
    number = jnp.arange(NBLK, dtype=jnp.int32)
    row_of = (2 * (number // N_GY) + number % 2).astype(jnp.int32)
    col_of = (number % N_GY // 2).astype(jnp.int32)
    grad_blocks = tiles[row_of, col_of]
    updates = lax.map(precondition, (grad_blocks, left_roots, right_roots))
    grid_rows = jnp.arange(row_blocks, dtype=jnp.int32)[:, None]
    grid_cols = jnp.arange(col_blocks, dtype=jnp.int32)[None, :]
    owner = (grid_rows // 2 * N_GY + 2 * grid_cols + grid_rows % 2).astype(jnp.int32)
    placed = updates[owner]
    return placed.transpose(0, 2, 1, 3).reshape(D, COLS)
```

```python
import functools

import jax
import jax.numpy as jnp
from jax import lax
from jax.experimental import pallas as pl
from jax.experimental.pallas import tpu as pltpu
from jax.sharding import PartitionSpec as P

epsilon = 1e-06
BF16 = jnp.bfloat16
F32 = jnp.float32
TOK = 1024
FEAT = 256
HALF = 512
BLK = 1024
GC = 2
OC = 4


def device(x, y, z, c):
    x, y, z = x % 4, y % 4, z % 4
    return ((x // 2) * 2 + c, (x % 2) * 16 + z * 4 + y)


def push(src, dst, send_sem, recv_sem, target):
    return pltpu.make_async_remote_copy(
        src_ref=src, dst_ref=dst, send_sem=send_sem, recv_sem=recv_sem,
        device_id=target, device_id_type=pl.DeviceIdType.MESH,
    )


def split(value):
    high = value.astype(BF16)
    return high, (value - high.astype(F32)).astype(BF16)


def mm(a, b):
    return jnp.dot(a, b, preferred_element_type=F32)


def kernel(
    act, cot, left, right, out,
    abuf, gbuf, l1, l2, r1, r2, sbuf, wbuf, gacc, g1, g2, gsq, ssq, fin,
    a_recv, x_send, y_send, up_send, down_send,
    g_recv, g_send, gf_send, gd_send, o_recv, o_send, od_send, l_sem, lg_sem, lo_sem,
):
    gx, gy = lax.axis_index("gx"), lax.axis_index("gy")
    x_hi, c = gx // 2, gx % 2
    x_lo, z, y = gy // 16, (gy // 4) % 4, gy % 4
    x = 2 * x_hi + x_lo
    p = y % 2
    y_pair = y + 1 - 2 * p
    odd = (y + z) % 2
    k_home = z // 2
    rel = (2 * c + p - z) % 4
    home = rel == 0
    other_core = device(x, y, z, 1 - c)
    across = device(x + 2, y, z, c)
    pair = device(x, y_pair, z, c)
    pair_across = device(x + 2, y_pair, z, c)

    load_left = pltpu.make_async_copy(left.at[0], sbuf, l_sem.at[0])
    load_right = pltpu.make_async_copy(right.at[0], wbuf, l_sem.at[1])
    load_left.start()
    load_right.start()

    barrier = pltpu.get_barrier_semaphore()
    greeted = [device(x + d, y, z, c) for d in (1, 2, 3)]
    greeted += [device(x, y + d, z, c) for d in (1, 2, 3)]
    greeted += [device(x, y + d, z, 1 - c) for d in (0, 1, 2, 3)]
    greeted += [device(x, y, z + 1, c), device(x, y, z + 3, c), pair_across]
    for target in greeted:
        pl.semaphore_signal(barrier, inc=1, device_id=target, device_id_type=pl.DeviceIdType.MESH)
    pl.semaphore_wait(barrier, len(greeted))

    def arrived(ref, sem):
        push(ref, ref, x_send.at[0], sem, other_core).wait_recv()

    keeps_home = jnp.logical_and(odd == 0, c == k_home)

    def x_slot(source):
        return jnp.where(keeps_home, 4 * y + 2 * source + c, 16 + source)

    own_slot = x_slot(x_hi)
    x_target = [2 * x_lo, 2 * x_lo + 1]
    for t in range(2):
        copy = push(act, abuf.at[own_slot], x_send.at[t], a_recv.at[own_slot], device(x_target[t], y, z, c))
        pl.when(x_target[t] != x)(copy.start)
    stays = pltpu.make_async_copy(act, abuf.at[own_slot], a_recv.at[own_slot])
    pl.when(x_lo == x_hi)(stays.start)

    g_own, g_far = 2 * x_hi + c, 2 * (1 - x_hi) + c
    rows = TOK // GC

    def g_part(g, h, j):
        return gbuf.at[g, h, pl.ds(rows * j, rows), :]

    def g_sem(g, h, j):
        return g_recv.at[(2 * g + h) * GC + j]

    keep_g = pltpu.make_async_copy(cot, gbuf.at[g_own, p], lg_sem)
    keep_g.start()
    g_sends = []
    for j in range(GC):
        for n, target in enumerate((pair, across, other_core)):
            copy = push(cot.at[pl.ds(rows * j, rows), :], g_part(g_own, p, j), g_send.at[n, j], g_sem(g_own, p, j), target)
            copy.start()
            g_sends.append(copy)

    y_copies = []
    for s in range(2):
        source = (x_hi + s) % 2
        slot = x_slot(source)
        arrived(abuf.at[slot], a_recv.at[slot])
        final = 4 * y + 2 * source + c
        for n, (when, dy) in enumerate(((odd == 1, 1), (odd == 1, 3), (odd == 0, 2))):
            copy = push(
                abuf.at[slot], abuf.at[final], y_send.at[n, s], a_recv.at[final], device(x, y + dy, z, k_home)
            )
            pl.when(when)(copy.start)
            y_copies.append((when, copy))
        copy = push(abuf.at[slot], abuf.at[final], y_send.at[3, s], a_recv.at[final], other_core)
        when = jnp.logical_and(odd == 0, c != k_home)
        pl.when(when)(copy.start)
        y_copies.append((when, copy))

    def split_roots(i, carry):
        part = pl.ds(pl.multiple_of(128 * i, 128), 128)
        l1[part, :], l2[part, :] = split(sbuf[part, :])
        r1[part, :], r2[part, :] = split(wbuf[part, :])
        return carry

    load_left.wait()
    load_right.wait()
    lax.fori_loop(0, 8, split_roots, 0)
    sbuf[...] = jnp.zeros_like(sbuf)
    gsq[...] = jnp.zeros_like(gsq)
    ssq[...] = jnp.zeros_like(ssq)

    above, below = device(x, y, z + 1, c), device(x, y, z + 3, c)

    def order(i):
        q = i // 4
        ys = (y + q + (q // 2) * (1 - 2 * (q % 2))) % 4
        g = 2 * ((x_hi + (i % 4) // 2) % 2) + i % 2
        return ys, g, 4 * ys + g

    def z_copies(i):
        _, _, slot = order(i)
        ref = abuf.at[slot]
        up = push(ref, ref, up_send.at[slot], a_recv.at[slot], above)
        down = push(ref, ref, down_send.at[slot], a_recv.at[slot], below)
        go_up = jnp.logical_or(home, jnp.logical_and(rel == 3, i % 2 == 0))
        go_down = jnp.logical_or(home, jnp.logical_and(rel == 1, i % 2 == 1))
        return (go_up, up), (go_down, down)

    def relay(i, carry=0):
        _, g, slot = order(i)
        held = jnp.logical_and(keeps_home, jnp.logical_and(i // 4 == 0, i % 2 == c))

        @pl.when(jnp.logical_not(held))
        def _():
            arrived(abuf.at[slot], a_recv.at[slot])

        for when, copy in z_copies(i):
            pl.when(when)(copy.start)
        return carry

    gf_sends, gd_sends = [], []

    def to_core(g, h, j):
        copy = push(g_part(g, h, j), g_part(g, h, j), gd_send.at[len(gd_sends)], g_sem(g, h, j), other_core)
        copy.start()
        gd_sends.append(copy)

    def cot_pair(j):
        arrived(g_part(g_own, 1 - p, j), g_sem(g_own, 1 - p, j))
        copy = push(g_part(g_own, 1 - p, j), g_part(g_own, 1 - p, j), gf_send.at[j], g_sem(g_own, 1 - p, j), across)
        copy.start()
        gf_sends.append(copy)
        to_core(g_own, 1 - p, j)

    def cot_far(h, j):
        arrived(g_part(g_far, h, j), g_sem(g_far, h, j))
        to_core(g_far, h, j)

    steps = [
        [0], [lambda: cot_pair(0)], [1, 2], [lambda: cot_pair(1), lambda: cot_far(p, 0)], [3, 4],
        [lambda: cot_far(p, 1)], [5, 6], [lambda: cot_far(1 - p, 0)], [7, 8], [lambda: cot_far(1 - p, 1)], [9],
    ]
    for group in steps:
        for step in group:
            if callable(step):
                step()
            else:
                relay(step)
    for g in range(2):
        for h in range(2):
            for j in range(GC):
                number = 2 * g + 1 - c
                arrived(g_part(number, h, j), g_sem(number, h, j))
    keep_g.wait()

    def piece(i, carry):
        ys, g, slot = order(i)

        @pl.when(i % 4 == 0)
        def _():
            gacc[...] = jnp.zeros_like(gacc)

        for h in range(2):
            gacc[:, pl.ds(HALF * h, HALF)] += lax.dot_general(
                abuf[slot], gbuf[g, h], (((0,), (0,)), ((), ())), preferred_element_type=F32
            )

        @pl.when(i % 4 == 3)
        def _():
            value = gacc[...]
            gsq[...] += jnp.sum(value * value, axis=0, keepdims=True)
            g1[...], g2[...] = split(value)
            columns = pl.ds(pl.multiple_of(FEAT * ys, FEAT), FEAT)

            def left_rows(r, inner):
                part = pl.ds(pl.multiple_of(256 * r, 256), 256)
                high = l1[part, columns]
                sbuf[part, :] += mm(high, g1[...]) + mm(high, g2[...]) + mm(l2[part, columns], g1[...])
                return inner

            lax.fori_loop(0, 4, left_rows, 0)

        return carry

    def relay_and_multiply(i, carry):
        relay(i)
        lax.fori_loop((i - 10) * 16 // 6, (i - 9) * 16 // 6, piece, 0)
        return carry

    lax.fori_loop(10, 16, relay_and_multiply, 0)

    def right_rows(r, carry):
        part = pl.ds(pl.multiple_of(256 * r, 256), 256)
        high, low = split(sbuf[part, :])
        for h in range(2):
            cols = pl.ds(HALF * h, HALF)
            value = mm(high, r1[:, cols]) + mm(high, r2[:, cols]) + mm(low, r1[:, cols])
            wbuf[part, cols] = value
            ssq[:, cols] += jnp.sum(value * value, axis=0, keepdims=True)
        return carry

    lax.fori_loop(0, 4, right_rows, 0)
    count = BLK * BLK
    graft = jnp.sqrt(jnp.sum(gsq[...], axis=1, keepdims=True) / count + epsilon) / jnp.sqrt(
        jnp.sum(ssq[...], axis=1, keepdims=True) / count + epsilon
    )

    block = 4 * x_hi + 2 * c + p
    orows = BLK // OC

    def o_part(number, j):
        return out.at[pl.ds(pl.multiple_of(BLK * number + orows * j, orows), orows), :]

    def o_sem(number, j):
        return o_recv.at[number * OC + j]

    o_sends = []
    for j in range(OC + 1):
        if j < OC:
            for h in range(2):
                fin[h, pl.ds(orows * j, orows), :] = (
                    wbuf[pl.ds(orows * j, orows), pl.ds(HALF * h, HALF)] * graft
                ).astype(BF16)
        if j > 0:
            i = j - 1
            mine = fin.at[p, pl.ds(orows * i, orows), :]
            theirs = fin.at[1 - p, pl.ds(orows * i, orows), :]
            for n, (src, target) in enumerate(
                ((mine, across), (theirs, pair_across), (theirs, pair), (mine, other_core))
            ):
                copy = push(src, o_part(block, i), o_send.at[n, i], o_sem(block, i), target)
                copy.start()
                o_sends.append(copy)
            copy = pltpu.make_async_copy(mine, o_part(block, i), lo_sem.at[i])
            copy.start()
    od_sends = []
    p_core = 2 * c
    far = 4 * (1 - x_hi)
    for j in range(OC):
        for n, number in enumerate((4 * x_hi + p_core + 1 - p, far + p_core + p, far + p_core + 1 - p)):
            arrived(o_part(number, j), o_sem(number, j))
            copy = push(o_part(number, j), o_part(number, j), od_send.at[n, j], o_sem(number, j), other_core)
            copy.start()
            od_sends.append(copy)

    for j in range(OC):
        for number in (0, 1, 4, 5):
            arrived(o_part(number + 2 * (1 - c), j), o_sem(number + 2 * (1 - c), j))
        pltpu.make_async_copy(fin.at[p, pl.ds(orows * j, orows), :], o_part(block, j), lo_sem.at[j]).wait()
    for t in range(2):
        copy = push(act, abuf.at[own_slot], x_send.at[t], a_recv.at[own_slot], device(x_target[t], y, z, c))
        pl.when(x_target[t] != x)(copy.wait_send)
    for when, copy in y_copies:
        pl.when(when)(copy.wait_send)

    def drain(i, carry):
        for when, copy in z_copies(i):
            pl.when(when)(copy.wait_send)
        return carry

    lax.fori_loop(0, 16, drain, 0)
    for copy in g_sends + gf_sends + gd_sends + o_sends + od_sends:
        copy.wait_send()


def local(act, cot, left, right):
    dma = pltpu.SemaphoreType.DMA
    anywhere = pl.BlockSpec(memory_space=pl.ANY)
    return pl.pallas_call(
        kernel,
        out_shape=jax.ShapeDtypeStruct((8 * BLK, HALF), BF16),
        in_specs=[anywhere] * 4,
        out_specs=anywhere,
        scratch_shapes=[
            pltpu.VMEM((18, TOK, FEAT), BF16),
            pltpu.VMEM((4, 2, TOK, HALF), BF16),
            pltpu.VMEM((BLK, BLK), BF16), pltpu.VMEM((BLK, BLK), BF16),
            pltpu.VMEM((BLK, BLK), BF16), pltpu.VMEM((BLK, BLK), BF16),
            pltpu.VMEM((BLK, BLK), F32), pltpu.VMEM((BLK, BLK), F32),
            pltpu.VMEM((FEAT, BLK), F32),
            pltpu.VMEM((FEAT, BLK), BF16), pltpu.VMEM((FEAT, BLK), BF16),
            pltpu.VMEM((1, BLK), F32), pltpu.VMEM((1, BLK), F32),
            pltpu.VMEM((2, BLK, HALF), BF16),
            dma((18,)), dma((2,)), dma((4, 2)), dma((16,)), dma((16,)),
            dma((8 * GC,)), dma((3, GC)), dma((GC,)), dma((3 * GC,)),
            dma((8 * OC,)), dma((4, OC)), dma((3, OC)), dma((2,)), dma, dma((OC,)),
        ],
        compiler_params=pltpu.CompilerParams(
            collective_id=0, has_side_effects=True, vmem_limit_bytes=62 * 1024 * 1024
        ),
        name="shampoo",
    )(act, cot, left, right)


def solution(mesh):
    in_specs = (P("gx", "gy"), P("gx", "gy"), P(("gx", "gy"), None, None), P(("gx", "gy"), None, None))
    return jax.shard_map(local, mesh=mesh, in_specs=in_specs, out_specs=P(None, "gy"), check_vma=False)
```

```python
import functools

import jax
import jax.numpy as jnp
from jax import lax
from jax.experimental import pallas as pl
from jax.experimental.pallas import tpu as pltpu
from jax.sharding import PartitionSpec as P

epsilon = 1e-06
BF16 = jnp.bfloat16
F32 = jnp.float32
TOK = 1024
FEAT = 256
HALF = 512
BLK = 1024
CH = 256
LAST = 3
GC = 4
OC = 4


def device(x, y, z, c):
    x, y, z = x % 4, y % 4, z % 4
    return ((x // 2) * 2 + c, (x % 2) * 16 + z * 4 + y)


def push(src, dst, send_sem, recv_sem, target):
    return pltpu.make_async_remote_copy(
        src_ref=src, dst_ref=dst, send_sem=send_sem, recv_sem=recv_sem,
        device_id=target, device_id_type=pl.DeviceIdType.MESH,
    )


def split(value):
    high = value.astype(BF16)
    return high, (value - high.astype(F32)).astype(BF16)


def mm(a, b):
    return jnp.dot(a, b, preferred_element_type=F32)


def kernel(
    act, cot, left, right, out,
    abuf, gbuf, l1, l2, r1, r2, sbuf, wbuf, gacc, g1, g2, gsq, ssq, fin,
    x_recv, x_send, y_send, a_recv, up_send, down_send, z_recv, z_send, t_recv, t_send,
    g_recv, g_send, gf_send, gd_send, o_recv, o_send, od_send, l_sem, lg_sem, lo_sem,
):
    gx, gy = lax.axis_index("gx"), lax.axis_index("gy")
    x_hi, c = gx // 2, gx % 2
    x_lo, z, y = gy // 16, (gy // 4) % 4, gy % 4
    x = 2 * x_hi + x_lo
    p = y % 2
    y_pair = y + 1 - 2 * p
    odd = (y + z) % 2
    k_home = z // 2
    mine_z = 2 * c + p
    rel = (mine_z - z) % 4
    home = rel == 0
    other_core = device(x, y, z, 1 - c)
    across = device(x + 2, y, z, c)
    pair = device(x, y_pair, z, c)
    pair_across = device(x + 2, y_pair, z, c)
    above, below = device(x, y, z + 1, c), device(x, y, z + 3, c)

    load_left = pltpu.make_async_copy(left.at[0], sbuf, l_sem.at[0])
    load_right = pltpu.make_async_copy(right.at[0], wbuf, l_sem.at[1])

    barrier = pltpu.get_barrier_semaphore()
    greeted = [device(x + d, y, z, c) for d in (1, 2, 3)]
    greeted += [device(x, y + d, z, c) for d in (1, 2, 3)]
    greeted += [device(x, y + d, z, 1 - c) for d in (0, 1, 2, 3)]
    greeted += [above, below, pair_across]
    for target in greeted:
        pl.semaphore_signal(barrier, inc=1, device_id=target, device_id_type=pl.DeviceIdType.MESH)
    pl.semaphore_wait(barrier, len(greeted))

    def arrived(ref, sem):
        push(ref, ref, x_send.at[0, 0], sem, other_core).wait_recv()

    finals = []

    def start(copy, when=None):
        if when is None:
            copy.start()
        else:
            pl.when(when)(copy.start)
        finals.append((when, copy))

    def a_rows(slot, t):
        return abuf.at[pl.ds(pl.multiple_of(TOK * slot + CH * t, CH), CH), :]

    def x_slot(source):
        return jnp.where(home, 4 * y + 2 * source + c, 16 + source)

    own_slot = x_slot(x_hi)
    for t in (LAST, 0, 1, 2):
        src = act.at[pl.ds(CH * t, CH), :]
        for n in range(2):
            target = 2 * x_lo + n
            start(
                push(src, a_rows(own_slot, t), x_send.at[n, t], x_recv.at[x_hi, t], device(target, y, z, c)),
                target != x,
            )
        stays = pltpu.make_async_copy(src, a_rows(own_slot, t), x_recv.at[x_hi, t])
        pl.when(x_lo == x_hi)(stays.start)

    g_own, g_far = 2 * x_hi + c, 2 * (1 - x_hi) + c

    def g_part(g, h, j):
        return gbuf.at[g, h, pl.ds(CH * j, CH), :]

    def g_sem(g, h, j):
        return g_recv.at[(2 * g + h) * GC + j]

    def cot_own(n, target, j):
        start(push(cot.at[pl.ds(CH * j, CH), :], g_part(g_own, p, j), g_send.at[n, j], g_sem(g_own, p, j), target))

    for j in range(GC):
        cot_own(0, across, j)
    for j in range(GC):
        cot_own(1, other_core, j)
    keep_g = pltpu.make_async_copy(cot, gbuf.at[g_own, p], lg_sem)
    keep_g.start()
    load_left.start()
    load_right.start()

    def t_rows(zs, source):
        final = TOK * (4 * y + 2 * source + c) + CH * LAST
        waits = jnp.where(zs == z, TOK * (16 + source) + CH * LAST, TOK * 18 + CH * (2 * zs + source))
        return abuf.at[pl.ds(pl.multiple_of(jnp.where(zs == mine_z, final, waits), CH), CH), :]

    def t_land(zs, source):
        final = TOK * (4 * y + 2 * source + c) + CH * LAST
        waits = TOK * 18 + CH * (2 * zs + source)
        return abuf.at[pl.ds(pl.multiple_of(jnp.where(zs == mine_z, final, waits), CH), CH), :]

    sources = [(x_hi + s) % 2 for s in range(2)]
    for s, source in enumerate(sources):
        arrived(a_rows(x_slot(source), LAST), x_recv.at[source, LAST])
        ref = t_rows(z, source)
        start(push(ref, t_land(z, source), z_send.at[0, s], z_recv.at[2 * z + source], above))
        start(push(ref, t_land(z, source), z_send.at[1, s], z_recv.at[2 * z + source], below))

    def along_y(t):
        for s, source in enumerate(sources):
            slot = x_slot(source)
            arrived(a_rows(slot, t), x_recv.at[source, t])
            final = 4 * y + 2 * source + c
            for n, (when, dy) in enumerate(((odd == 1, 1), (odd == 1, 3), (odd == 0, 2))):
                start(
                    push(
                        a_rows(slot, t), a_rows(final, t), y_send.at[n, s, t], a_recv.at[final * 3 + t],
                        device(x, y + dy, z, k_home),
                    ),
                    when,
                )
            start(
                push(a_rows(slot, t), a_rows(final, t), y_send.at[3, s, t], a_recv.at[final * 3 + t], other_core),
                jnp.logical_and(odd == 0, c != k_home),
            )

    def source_y(q):
        return (y + q + (q // 2) * (1 - 2 * (q % 2))) % 4

    def order(i):
        t, q = i // 16, (i // 4) % 4
        g = 2 * ((x_hi + (i % 4) // 2) % 2) + i % 2
        return t, q, 4 * source_y(q) + g

    def z_copies(i):
        t, _, slot = order(i)
        ref, number = a_rows(slot, t), slot * 3 + t
        up = push(ref, ref, up_send.at[number], a_recv.at[number], above)
        down = push(ref, ref, down_send.at[number], a_recv.at[number], below)
        go_up = jnp.logical_or(home, jnp.logical_and(rel == 3, i % 2 == 0))
        go_down = jnp.logical_or(home, jnp.logical_and(rel == 1, i % 2 == 1))
        return (go_up, up), (go_down, down)

    def relay(i, carry=0):
        t, q, slot = order(i)
        held = jnp.logical_and(home, jnp.logical_and(q == 0, i % 2 == c))

        @pl.when(jnp.logical_not(held))
        def _():
            arrived(a_rows(slot, t), a_recv.at[slot * 3 + t])

        for when, copy in z_copies(i):
            pl.when(when)(copy.start)
        return carry

    def relay_step(s):
        lax.fori_loop(4 * s, 4 * s + 4, relay, 0)

    def last_along_z():
        for s, (zs, source, target) in enumerate((((z + 3) % 4, 0, above), ((z + 1) % 4, 1, below))):
            ref = t_rows(zs, source)
            arrived(ref, z_recv.at[2 * zs + source])
            start(push(ref, t_land(zs, source), z_send.at[2, s], z_recv.at[2 * zs + source], target))

    def last_along_y():
        for zs, source in (((z + 3) % 4, 1), ((z + 1) % 4, 0), ((z + 2) % 4, 0), ((z + 2) % 4, 1)):
            arrived(t_rows(zs, source), z_recv.at[2 * zs + source])
        for source in range(2):
            final = 4 * y + 2 * source + c
            land = a_rows(final, LAST)
            near, there = 2 * c + p, 2 * (1 - c) + p
            near_odd, there_odd = 2 * c + 1 - p, 2 * (1 - c) + 1 - p
            for n, (zs, target) in enumerate((
                (there, other_core),
                (near_odd, device(x, y + 1, z, c)), (near_odd, device(x, y + 3, z, c)),
                (there_odd, device(x, y + 1, z, 1 - c)), (there_odd, device(x, y + 3, z, 1 - c)),
                (near, device(x, y + 2, z, c)), (there, device(x, y + 2, z, 1 - c)),
            )):
                start(push(t_rows(zs, source), land, t_send.at[source, n], t_recv.at[final], target))

    gd_count = [0]

    def to_core(g, h, j):
        start(push(g_part(g, h, j), g_part(g, h, j), gd_send.at[gd_count[0]], g_sem(g, h, j), other_core))
        gd_count[0] += 1

    def cot_pair(j):
        arrived(g_part(g_own, 1 - p, j), g_sem(g_own, 1 - p, j))
        start(push(g_part(g_own, 1 - p, j), g_part(g_own, 1 - p, j), gf_send.at[j], g_sem(g_own, 1 - p, j), across))
        to_core(g_own, 1 - p, j)

    def cot_far(h, j):
        arrived(g_part(g_far, h, j), g_sem(g_far, h, j))
        to_core(g_far, h, j)

    def from_core(h):
        for g in range(2):
            for j in range(GC):
                arrived(g_part(2 * g + 1 - c, h, j), g_sem(2 * g + 1 - c, h, j))

    def split_roots(i, carry):
        part = pl.ds(pl.multiple_of(128 * i, 128), 128)
        l1[part, :], l2[part, :] = split(sbuf[part, :])
        r1[part, :], r2[part, :] = split(wbuf[part, :])
        return carry

    def multiply(t, q, h):
        ys = source_y(q)
        value = None
        for g in range(4):
            product = lax.dot_general(
                abuf[pl.ds(pl.multiple_of(TOK * (4 * ys + g) + CH * t, CH), CH), :],
                gbuf[g, h, pl.ds(pl.multiple_of(CH * t, CH), CH), :],
                (((0,), (0,)), ((), ())), preferred_element_type=F32,
            )
            value = product if value is None else value + product
        gacc[pl.ds(pl.multiple_of(FEAT * ys, FEAT), FEAT), pl.ds(pl.multiple_of(HALF * h, HALF), HALF)] += value

    def multiply_early(h):
        def body(i, carry):
            multiply(i // 4, i % 4, h)
            return carry

        return body

    along_y(0)
    cot_own(2, pair, 0)
    cot_own(2, pair, 1)
    relay_step(0)
    along_y(1)
    cot_own(2, pair, 2)
    cot_own(2, pair, 3)
    last_along_z()
    along_y(2)
    load_left.wait()
    load_right.wait()
    lax.fori_loop(0, 8, split_roots, 0)
    relay_step(1)
    last_along_y()
    sbuf[...] = jnp.zeros_like(sbuf)
    gacc[...] = jnp.zeros_like(gacc)
    gsq[...] = jnp.zeros_like(gsq)
    ssq[...] = jnp.zeros_like(ssq)
    relay_step(2)
    cot_far(p, 0)
    cot_pair(0)
    relay_step(3)
    cot_far(p, 1)
    cot_pair(1)
    relay_step(4)
    cot_far(p, 2)
    relay_step(5)
    cot_far(p, 3)
    relay_step(6)
    cot_pair(2)
    cot_far(1 - p, 0)
    relay_step(7)
    cot_pair(3)
    cot_far(1 - p, 1)
    from_core(p)
    keep_g.wait()
    lax.fori_loop(0, 4, multiply_early(p), 0)
    relay_step(8)
    cot_far(1 - p, 2)
    lax.fori_loop(4, 8, multiply_early(p), 0)
    cot_far(1 - p, 3)
    from_core(1 - p)

    def last_steps(u, carry):
        @pl.when(u < 12)
        def _():
            relay(36 + u)

        lax.fori_loop(jnp.minimum(3 * u, 8), jnp.minimum(3 * u + 3, 8), multiply_early(1 - p), 0)
        q = (u + 1) // 3 - 1
        done = jnp.logical_or(jnp.logical_or(u == 3, u == 5), jnp.logical_or(u == 8, u == 12))

        @pl.when(done)
        def _():
            ys = source_y(q)
            for g in range(4):
                @pl.when(jnp.logical_not(jnp.logical_and(q == 0, c == g % 2)))
                def _():
                    arrived(a_rows(4 * ys + g, LAST), t_recv.at[4 * ys + g])

            def body(i, inner):
                multiply(2 + i // 2, q, i % 2)
                return inner

            lax.fori_loop(0, 4, body, 0)

        at = jnp.logical_or(jnp.logical_or(u == 4, u == 6), jnp.logical_or(u == 9, u == 12))
        @pl.when(at)
        def _():
            q2 = u // 3 - 1
            ys = source_y(q2)
            columns = pl.ds(pl.multiple_of(FEAT * ys, FEAT), FEAT)
            value = gacc[columns, :]
            gsq[...] += jnp.sum(value * value, axis=0, keepdims=True)
            g1[...], g2[...] = split(value)

            def left_rows(r, inner):
                part = pl.ds(pl.multiple_of(256 * r, 256), 256)
                high = l1[part, columns]
                sbuf[part, :] += mm(high, g1[...]) + mm(high, g2[...]) + mm(l2[part, columns], g1[...])
                return inner

            lax.fori_loop(0, 4, left_rows, 0)

        return carry

    lax.fori_loop(0, 13, last_steps, 0)

    def right_rows(r, carry):
        part = pl.ds(pl.multiple_of(256 * r, 256), 256)
        high, low = split(sbuf[part, :])
        for h in range(2):
            cols = pl.ds(HALF * h, HALF)
            value = mm(high, r1[:, cols]) + mm(high, r2[:, cols]) + mm(low, r1[:, cols])
            wbuf[part, cols] = value
            ssq[:, cols] += jnp.sum(value * value, axis=0, keepdims=True)
        return carry

    lax.fori_loop(0, 4, right_rows, 0)
    count = BLK * BLK
    graft = jnp.sqrt(jnp.sum(gsq[...], axis=1, keepdims=True) / count + epsilon) / jnp.sqrt(
        jnp.sum(ssq[...], axis=1, keepdims=True) / count + epsilon
    )

    block = 4 * x_hi + 2 * c + p
    orows = BLK // OC

    def o_part(number, j):
        return out.at[pl.ds(pl.multiple_of(BLK * number + orows * j, orows), orows), :]

    def o_sem(number, j):
        return o_recv.at[number * OC + j]

    for j in range(OC + 1):
        if j < OC:
            for h in range(2):
                fin[h, pl.ds(orows * j, orows), :] = (
                    wbuf[pl.ds(orows * j, orows), pl.ds(HALF * h, HALF)] * graft
                ).astype(BF16)
        if j > 0:
            i = j - 1
            mine = fin.at[p, pl.ds(orows * i, orows), :]
            theirs = fin.at[1 - p, pl.ds(orows * i, orows), :]
            for n, (src, target) in enumerate(
                ((mine, across), (theirs, pair_across), (theirs, pair), (mine, other_core))
            ):
                start(push(src, o_part(block, i), o_send.at[n, i], o_sem(block, i), target))
            copy = pltpu.make_async_copy(mine, o_part(block, i), lo_sem.at[i])
            copy.start()
    p_core = 2 * c
    far = 4 * (1 - x_hi)
    for j in range(OC):
        for n, number in enumerate((4 * x_hi + p_core + 1 - p, far + p_core + p, far + p_core + 1 - p)):
            arrived(o_part(number, j), o_sem(number, j))
            start(push(o_part(number, j), o_part(number, j), od_send.at[n, j], o_sem(number, j), other_core))

    for j in range(OC):
        for number in (0, 1, 4, 5):
            arrived(o_part(number + 2 * (1 - c), j), o_sem(number + 2 * (1 - c), j))
        pltpu.make_async_copy(fin.at[p, pl.ds(orows * j, orows), :], o_part(block, j), lo_sem.at[j]).wait()
    for when, copy in finals:
        if when is None:
            copy.wait_send()
        else:
            pl.when(when)(copy.wait_send)

    def drain(i, carry):
        for when, copy in z_copies(i):
            pl.when(when)(copy.wait_send)
        return carry

    lax.fori_loop(0, 48, drain, 0)


def local(act, cot, left, right):
    dma = pltpu.SemaphoreType.DMA
    anywhere = pl.BlockSpec(memory_space=pl.ANY)
    return pl.pallas_call(
        kernel,
        out_shape=jax.ShapeDtypeStruct((8 * BLK, HALF), BF16),
        in_specs=[anywhere] * 4,
        out_specs=anywhere,
        scratch_shapes=[
            pltpu.VMEM((20 * TOK, FEAT), BF16),
            pltpu.VMEM((4, 2, TOK, HALF), BF16),
            pltpu.VMEM((BLK, BLK), BF16), pltpu.VMEM((BLK, BLK), BF16),
            pltpu.VMEM((BLK, BLK), BF16), pltpu.VMEM((BLK, BLK), BF16),
            pltpu.VMEM((BLK, BLK), F32), pltpu.VMEM((BLK, BLK), F32),
            pltpu.VMEM((BLK, BLK), F32),
            pltpu.VMEM((FEAT, BLK), BF16), pltpu.VMEM((FEAT, BLK), BF16),
            pltpu.VMEM((1, BLK), F32), pltpu.VMEM((1, BLK), F32),
            pltpu.VMEM((2, BLK, HALF), BF16),
            dma((2, 4)), dma((2, 4)), dma((4, 2, 3)), dma((48,)), dma((48,)), dma((48,)),
            dma((8,)), dma((3, 2)), dma((16,)), dma((2, 7)),
            dma((8 * GC,)), dma((3, GC)), dma((GC,)), dma((3 * GC,)),
            dma((8 * OC,)), dma((4, OC)), dma((3, OC)), dma((2,)), dma, dma((OC,)),
        ],
        compiler_params=pltpu.CompilerParams(
            collective_id=0, has_side_effects=True, vmem_limit_bytes=62 * 1024 * 1024
        ),
        name="shampoo",
    )(act, cot, left, right)


def solution(mesh):
    in_specs = (P("gx", "gy"), P("gx", "gy"), P(("gx", "gy"), None, None), P(("gx", "gy"), None, None))
    return jax.shard_map(local, mesh=mesh, in_specs=in_specs, out_specs=P(None, "gy"), check_vma=False)
```

```python
import functools

import jax
import jax.numpy as jnp
from jax import lax
from jax.experimental import pallas as pl
from jax.experimental.pallas import tpu as pltpu
from jax.sharding import PartitionSpec as P

epsilon = 1e-06
BF16 = jnp.bfloat16
F32 = jnp.float32
TOK = 1024
FEAT = 256
HALF = 512
BLK = 1024
CH = 256
LAST = 3
GC = 4
OC = 4


def device(x, y, z, c):
    x, y, z = x % 4, y % 4, z % 4
    return ((x // 2) * 2 + c, (x % 2) * 16 + z * 4 + y)


def push(src, dst, send_sem, recv_sem, target):
    return pltpu.make_async_remote_copy(
        src_ref=src, dst_ref=dst, send_sem=send_sem, recv_sem=recv_sem,
        device_id=target, device_id_type=pl.DeviceIdType.MESH,
    )


def split(value):
    high = value.astype(BF16)
    return high, (value - high.astype(F32)).astype(BF16)


def mm(a, b):
    return jnp.dot(a, b, preferred_element_type=F32)


def kernel(
    act, cot, left, right, out,
    abuf, gbuf, l1, l2, r1, r2, sbuf, wbuf, gacc, g1, g2, gsq, ssq, fin,
    x_recv, x_send, y_send, a_recv, up_send, down_send, z_recv, z_send, t_recv, t_send,
    g_recv, g_send, gf_send, gd_send, o_recv, o_send, od_send, l_sem, lg_sem, lo_sem,
):
    gx, gy = lax.axis_index("gx"), lax.axis_index("gy")
    x_hi, c = gx // 2, gx % 2
    x_lo, z, y = gy // 16, (gy // 4) % 4, gy % 4
    x = 2 * x_hi + x_lo
    p = y % 2
    y_pair = y + 1 - 2 * p
    odd = (y + z) % 2
    k_home = z // 2
    mine_z = 2 * c + p
    rel = (mine_z - z) % 4
    home = rel == 0
    other_core = device(x, y, z, 1 - c)
    across = device(x + 2, y, z, c)
    pair = device(x, y_pair, z, c)
    pair_across = device(x + 2, y_pair, z, c)
    above, below = device(x, y, z + 1, c), device(x, y, z + 3, c)

    load_left = pltpu.make_async_copy(left.at[0], sbuf, l_sem.at[0])
    load_right = pltpu.make_async_copy(right.at[0], wbuf, l_sem.at[1])

    barrier = pltpu.get_barrier_semaphore()
    greeted = [device(x + d, y, z, c) for d in (1, 2, 3)]
    greeted += [device(x, y + d, z, c) for d in (1, 2, 3)]
    greeted += [device(x, y + d, z, 1 - c) for d in (0, 1, 2, 3)]
    greeted += [above, below, pair_across]
    for target in greeted:
        pl.semaphore_signal(barrier, inc=1, device_id=target, device_id_type=pl.DeviceIdType.MESH)
    pl.semaphore_wait(barrier, len(greeted))

    def arrived(ref, sem):
        push(ref, ref, x_send.at[0, 0], sem, other_core).wait_recv()

    finals = []

    def start(copy, when=None):
        if when is None:
            copy.start()
        else:
            pl.when(when)(copy.start)
        finals.append((when, copy))

    def a_rows(slot, t):
        return abuf.at[pl.ds(pl.multiple_of(TOK * slot + CH * t, CH), CH), :]

    def x_slot(source):
        return jnp.where(home, 4 * y + 2 * source + c, 16 + source)

    own_slot = x_slot(x_hi)
    for t in (LAST, 0, 1, 2):
        src = act.at[pl.ds(CH * t, CH), :]
        for n in range(2):
            target = 2 * x_lo + n
            start(
                push(src, a_rows(own_slot, t), x_send.at[n, t], x_recv.at[x_hi, t], device(target, y, z, c)),
                target != x,
            )
        stays = pltpu.make_async_copy(src, a_rows(own_slot, t), x_recv.at[x_hi, t])
        pl.when(x_lo == x_hi)(stays.start)

    g_own, g_far = 2 * x_hi + c, 2 * (1 - x_hi) + c

    def g_part(g, h, j):
        return gbuf.at[g, h, pl.ds(CH * j, CH), :]

    def g_sem(g, h, j):
        return g_recv.at[(2 * g + h) * GC + j]

    def cot_own(n, target, j):
        start(push(cot.at[pl.ds(CH * j, CH), :], g_part(g_own, p, j), g_send.at[n, j], g_sem(g_own, p, j), target))

    for j in range(GC):
        cot_own(0, across, j)
    for j in range(GC):
        cot_own(1, other_core, j)
    keep_g = pltpu.make_async_copy(cot, gbuf.at[g_own, p], lg_sem)
    keep_g.start()
    load_left.start()
    load_right.start()

    def t_rows(zs, source):
        final = TOK * (4 * y + 2 * source + c) + CH * LAST
        waits = jnp.where(zs == z, TOK * (16 + source) + CH * LAST, TOK * 18 + CH * (2 * zs + source))
        return abuf.at[pl.ds(pl.multiple_of(jnp.where(zs == mine_z, final, waits), CH), CH), :]

    def t_land(zs, source):
        final = TOK * (4 * y + 2 * source + c) + CH * LAST
        waits = TOK * 18 + CH * (2 * zs + source)
        return abuf.at[pl.ds(pl.multiple_of(jnp.where(zs == mine_z, final, waits), CH), CH), :]

    sources = [(x_hi + s) % 2 for s in range(2)]
    for s, source in enumerate(sources):
        arrived(a_rows(x_slot(source), LAST), x_recv.at[source, LAST])
        ref = t_rows(z, source)
        start(push(ref, t_land(z, source), z_send.at[0, s], z_recv.at[2 * z + source], above))
        start(push(ref, t_land(z, source), z_send.at[1, s], z_recv.at[2 * z + source], below))

    def along_y(t):
        for s, source in enumerate(sources):
            slot = x_slot(source)
            arrived(a_rows(slot, t), x_recv.at[source, t])
            for _, copy in z_copies(4 * t + 2 * s + c):
                pl.when(home)(copy.start)
            final = 4 * y + 2 * source + c
            for n, (when, dy) in enumerate(((odd == 1, 1), (odd == 1, 3), (odd == 0, 2))):
                start(
                    push(
                        a_rows(slot, t), a_rows(final, t), y_send.at[n, s, t], a_recv.at[final * 3 + t],
                        device(x, y + dy, z, k_home),
                    ),
                    when,
                )
            start(
                push(a_rows(slot, t), a_rows(final, t), y_send.at[3, s, t], a_recv.at[final * 3 + t], other_core),
                jnp.logical_and(odd == 0, c != k_home),
            )

    def source_y(q):
        return (y + q + (q // 2) * (1 - 2 * (q % 2))) % 4

    def step_of(step):
        own = step < 3
        rest = jnp.maximum(step - 3, 0)
        return jnp.where(own, step, rest // 3), jnp.where(own, 0, 1 + rest % 3)

    def order(i):
        t, q = step_of(i // 4)
        g = 2 * ((x_hi + (i % 4) // 2) % 2) + i % 2
        return t, q, 4 * source_y(q) + g

    def z_copies(i):
        t, _, slot = order(i)
        ref, number = a_rows(slot, t), slot * 3 + t
        up = push(ref, ref, up_send.at[number], a_recv.at[number], above)
        down = push(ref, ref, down_send.at[number], a_recv.at[number], below)
        go_up = jnp.logical_or(home, jnp.logical_and(rel == 3, i % 2 == 0))
        go_down = jnp.logical_or(home, jnp.logical_and(rel == 1, i % 2 == 1))
        return (go_up, up), (go_down, down)

    def relay(i, carry=0):
        t, q, slot = order(i)
        held = jnp.logical_and(home, jnp.logical_and(q == 0, i % 2 == c))

        @pl.when(jnp.logical_not(held))
        def _():
            arrived(a_rows(slot, t), a_recv.at[slot * 3 + t])
            for when, copy in z_copies(i):
                pl.when(when)(copy.start)

        return carry

    def relay_step(s):
        lax.fori_loop(4 * s, 4 * s + 4, relay, 0)

    def last_along_z():
        for s, (zs, source, target) in enumerate((((z + 3) % 4, 0, above), ((z + 1) % 4, 1, below))):
            ref = t_rows(zs, source)
            arrived(ref, z_recv.at[2 * zs + source])
            start(push(ref, t_land(zs, source), z_send.at[2, s], z_recv.at[2 * zs + source], target))

    def last_along_y():
        for zs, source in (((z + 3) % 4, 1), ((z + 1) % 4, 0), ((z + 2) % 4, 0), ((z + 2) % 4, 1)):
            arrived(t_rows(zs, source), z_recv.at[2 * zs + source])
        for source in range(2):
            final = 4 * y + 2 * source + c
            land = a_rows(final, LAST)
            near, there = 2 * c + p, 2 * (1 - c) + p
            near_odd, there_odd = 2 * c + 1 - p, 2 * (1 - c) + 1 - p
            for n, (zs, target) in enumerate((
                (there, other_core),
                (near_odd, device(x, y + 1, z, c)), (near_odd, device(x, y + 3, z, c)),
                (there_odd, device(x, y + 1, z, 1 - c)), (there_odd, device(x, y + 3, z, 1 - c)),
                (near, device(x, y + 2, z, c)), (there, device(x, y + 2, z, 1 - c)),
            )):
                start(push(t_rows(zs, source), land, t_send.at[source, n], t_recv.at[final], target))

    gd_count = [0]

    def to_core(g, h, j):
        start(push(g_part(g, h, j), g_part(g, h, j), gd_send.at[gd_count[0]], g_sem(g, h, j), other_core))
        gd_count[0] += 1

    def cot_pair(j):
        arrived(g_part(g_own, 1 - p, j), g_sem(g_own, 1 - p, j))
        start(push(g_part(g_own, 1 - p, j), g_part(g_own, 1 - p, j), gf_send.at[j], g_sem(g_own, 1 - p, j), across))
        to_core(g_own, 1 - p, j)

    def cot_far(h, j):
        arrived(g_part(g_far, h, j), g_sem(g_far, h, j))
        to_core(g_far, h, j)

    def from_core(h):
        for g in range(2):
            for j in range(GC):
                arrived(g_part(2 * g + 1 - c, h, j), g_sem(2 * g + 1 - c, h, j))

    def split_roots(i, carry):
        part = pl.ds(pl.multiple_of(128 * i, 128), 128)
        l1[part, :], l2[part, :] = split(sbuf[part, :])
        r1[part, :], r2[part, :] = split(wbuf[part, :])
        return carry

    def multiply(t, q, h):
        ys = source_y(q)
        value = None
        for g in range(4):
            product = lax.dot_general(
                abuf[pl.ds(pl.multiple_of(TOK * (4 * ys + g) + CH * t, CH), CH), :],
                gbuf[g, h, pl.ds(pl.multiple_of(CH * t, CH), CH), :],
                (((0,), (0,)), ((), ())), preferred_element_type=F32,
            )
            value = product if value is None else value + product
        gacc[pl.ds(pl.multiple_of(FEAT * ys, FEAT), FEAT), pl.ds(pl.multiple_of(HALF * h, HALF), HALF)] += value

    def multiply_early(h):
        def body(i, carry):
            multiply(*step_of(i), h)
            return carry

        return body

    along_y(0)
    cot_own(2, pair, 0)
    cot_own(2, pair, 1)
    along_y(1)
    cot_own(2, pair, 2)
    cot_own(2, pair, 3)
    along_y(2)
    last_along_z()
    relay_step(0)
    relay_step(1)
    last_along_y()
    cot_far(p, 0)
    cot_pair(0)
    load_left.wait()
    load_right.wait()
    lax.fori_loop(0, 8, split_roots, 0)
    relay_step(2)
    cot_far(p, 1)
    cot_pair(1)
    cot_far(p, 2)
    sbuf[...] = jnp.zeros_like(sbuf)
    gacc[...] = jnp.zeros_like(gacc)
    gsq[...] = jnp.zeros_like(gsq)
    ssq[...] = jnp.zeros_like(ssq)
    relay_step(3)
    cot_far(p, 3)
    relay_step(4)
    cot_pair(2)
    cot_far(1 - p, 0)
    relay_step(5)
    cot_pair(3)
    cot_far(1 - p, 1)
    from_core(p)
    keep_g.wait()
    relay_step(6)
    cot_far(1 - p, 2)
    lax.fori_loop(0, 4, multiply_early(p), 0)
    relay_step(7)
    cot_far(1 - p, 3)
    lax.fori_loop(4, 8, multiply_early(p), 0)
    relay_step(8)
    lax.fori_loop(8, 9, multiply_early(p), 0)
    from_core(1 - p)

    def last_steps(u, carry):
        @pl.when(u < 12)
        def _():
            relay(36 + u)

        lax.fori_loop(jnp.minimum(3 * u, 9), jnp.minimum(3 * u + 3, 9), multiply_early(1 - p), 0)
        q = (u + 1) // 3 - 1
        done = jnp.logical_or(jnp.logical_or(u == 3, u == 5), jnp.logical_or(u == 8, u == 12))

        @pl.when(done)
        def _():
            ys = source_y(q)
            for g in range(4):
                @pl.when(jnp.logical_not(jnp.logical_and(q == 0, c == g % 2)))
                def _():
                    arrived(a_rows(4 * ys + g, LAST), t_recv.at[4 * ys + g])

            def body(i, inner):
                multiply(2 + i // 2, q, i % 2)
                return inner

            lax.fori_loop(jnp.where(q == 0, 2, 0), 4, body, 0)

        at = jnp.logical_or(jnp.logical_or(u == 4, u == 6), jnp.logical_or(u == 9, u == 12))
        @pl.when(at)
        def _():
            q2 = u // 3 - 1
            ys = source_y(q2)
            columns = pl.ds(pl.multiple_of(FEAT * ys, FEAT), FEAT)
            value = gacc[columns, :]
            gsq[...] += jnp.sum(value * value, axis=0, keepdims=True)
            g1[...], g2[...] = split(value)

            def left_rows(r, inner):
                part = pl.ds(pl.multiple_of(256 * r, 256), 256)
                high = l1[part, columns]
                sbuf[part, :] += mm(high, g1[...]) + mm(high, g2[...]) + mm(l2[part, columns], g1[...])
                return inner

            lax.fori_loop(0, 4, left_rows, 0)

        return carry

    lax.fori_loop(0, 13, last_steps, 0)

    def right_rows(r, carry):
        part = pl.ds(pl.multiple_of(256 * r, 256), 256)
        high, low = split(sbuf[part, :])
        for h in range(2):
            cols = pl.ds(HALF * h, HALF)
            value = mm(high, r1[:, cols]) + mm(high, r2[:, cols]) + mm(low, r1[:, cols])
            wbuf[part, cols] = value
            ssq[:, cols] += jnp.sum(value * value, axis=0, keepdims=True)
        return carry

    lax.fori_loop(0, 4, right_rows, 0)
    count = BLK * BLK
    graft = jnp.sqrt(jnp.sum(gsq[...], axis=1, keepdims=True) / count + epsilon) / jnp.sqrt(
        jnp.sum(ssq[...], axis=1, keepdims=True) / count + epsilon
    )

    block = 4 * x_hi + 2 * c + p
    orows = BLK // OC

    def o_part(number, j):
        return out.at[pl.ds(pl.multiple_of(BLK * number + orows * j, orows), orows), :]

    def o_sem(number, j):
        return o_recv.at[number * OC + j]

    for j in range(OC + 1):
        if j < OC:
            for h in range(2):
                fin[h, pl.ds(orows * j, orows), :] = (
                    wbuf[pl.ds(orows * j, orows), pl.ds(HALF * h, HALF)] * graft
                ).astype(BF16)
        if j > 0:
            i = j - 1
            mine = fin.at[p, pl.ds(orows * i, orows), :]
            theirs = fin.at[1 - p, pl.ds(orows * i, orows), :]
            for n, (src, target) in enumerate(
                ((mine, across), (theirs, pair_across), (theirs, pair), (mine, other_core))
            ):
                start(push(src, o_part(block, i), o_send.at[n, i], o_sem(block, i), target))
            copy = pltpu.make_async_copy(mine, o_part(block, i), lo_sem.at[i])
            copy.start()
    p_core = 2 * c
    far = 4 * (1 - x_hi)
    for j in range(OC):
        for n, number in enumerate((4 * x_hi + p_core + 1 - p, far + p_core + p, far + p_core + 1 - p)):
            arrived(o_part(number, j), o_sem(number, j))
            start(push(o_part(number, j), o_part(number, j), od_send.at[n, j], o_sem(number, j), other_core))

    for j in range(OC):
        for number in (0, 1, 4, 5):
            arrived(o_part(number + 2 * (1 - c), j), o_sem(number + 2 * (1 - c), j))
        pltpu.make_async_copy(fin.at[p, pl.ds(orows * j, orows), :], o_part(block, j), lo_sem.at[j]).wait()
    for when, copy in finals:
        if when is None:
            copy.wait_send()
        else:
            pl.when(when)(copy.wait_send)

    def drain(i, carry):
        for when, copy in z_copies(i):
            pl.when(when)(copy.wait_send)
        return carry

    lax.fori_loop(0, 48, drain, 0)


def local(act, cot, left, right):
    dma = pltpu.SemaphoreType.DMA
    anywhere = pl.BlockSpec(memory_space=pl.ANY)
    return pl.pallas_call(
        kernel,
        out_shape=pltpu.VMEM((8 * BLK, HALF), BF16),
        in_specs=[anywhere] * 4,
        out_specs=anywhere,
        scratch_shapes=[
            pltpu.VMEM((20 * TOK, FEAT), BF16),
            pltpu.VMEM((4, 2, TOK, HALF), BF16),
            pltpu.VMEM((BLK, BLK), BF16), pltpu.VMEM((BLK, BLK), BF16),
            pltpu.VMEM((BLK, BLK), BF16), pltpu.VMEM((BLK, BLK), BF16),
            pltpu.VMEM((BLK, BLK), F32), pltpu.VMEM((BLK, BLK), F32),
            pltpu.VMEM((BLK, BLK), F32),
            pltpu.VMEM((FEAT, BLK), BF16), pltpu.VMEM((FEAT, BLK), BF16),
            pltpu.VMEM((1, BLK), F32), pltpu.VMEM((1, BLK), F32),
            pltpu.VMEM((2, BLK, HALF), BF16),
            dma((2, 4)), dma((2, 4)), dma((4, 2, 3)), dma((48,)), dma((48,)), dma((48,)),
            dma((8,)), dma((3, 2)), dma((16,)), dma((2, 7)),
            dma((8 * GC,)), dma((3, GC)), dma((GC,)), dma((3 * GC,)),
            dma((8 * OC,)), dma((4, OC)), dma((3, OC)), dma((2,)), dma, dma((OC,)),
        ],
        compiler_params=pltpu.CompilerParams(
            collective_id=0, has_side_effects=True, vmem_limit_bytes=46 * 1024 * 1024
        ),
        name="shampoo",
    )(act, cot, left, right)


def solution(mesh):
    in_specs = (P("gx", "gy"), P("gx", "gy"), P(("gx", "gy"), None, None), P(("gx", "gy"), None, None))
    return jax.shard_map(local, mesh=mesh, in_specs=in_specs, out_specs=P(None, "gy"), check_vma=False)
```

```python
import functools

import jax
import jax.numpy as jnp
from jax import lax
from jax.experimental import pallas as pl
from jax.experimental.pallas import tpu as pltpu
from jax.sharding import PartitionSpec as P

epsilon = 1e-06
BF16 = jnp.bfloat16
F32 = jnp.float32
TOK = 1024
FEAT = 256
HALF = 512
BLK = 1024
CH = 256
LAST = 3
GC = 4
OC = 4


def device(x, y, z, c):
    x, y, z = x % 4, y % 4, z % 4
    return ((x // 2) * 2 + c, (x % 2) * 16 + z * 4 + y)


def push(src, dst, send_sem, recv_sem, target):
    return pltpu.make_async_remote_copy(
        src_ref=src, dst_ref=dst, send_sem=send_sem, recv_sem=recv_sem,
        device_id=target, device_id_type=pl.DeviceIdType.MESH,
    )


def split(value):
    high = value.astype(BF16)
    return high, (value - high.astype(F32)).astype(BF16)


def mm(a, b):
    return jnp.dot(a, b, preferred_element_type=F32)


def kernel(
    act, cot, left, right, out,
    abuf, gbuf, l1, l2, r1, r2, sbuf, wbuf, gacc, g1, g2, gsq, ssq, fin,
    x_recv, x_send, y_send, a_recv, up_send, down_send, z_recv, z_send, t_recv, t_send,
    g_recv, g_send, gf_send, gd_send, o_recv, o_send, od_send, l_sem, lg_sem, lo_sem,
):
    gx, gy = lax.axis_index("gx"), lax.axis_index("gy")
    x_hi, c = gx // 2, gx % 2
    x_lo, z, y = gy // 16, (gy // 4) % 4, gy % 4
    x = 2 * x_hi + x_lo
    p = y % 2
    y_pair = y + 1 - 2 * p
    odd = (y + z) % 2
    k_home = z // 2
    mine_z = 2 * c + p
    rel = (mine_z - z) % 4
    home = rel == 0
    other_core = device(x, y, z, 1 - c)
    across = device(x + 2, y, z, c)
    pair = device(x, y_pair, z, c)
    pair_across = device(x + 2, y_pair, z, c)
    above, below = device(x, y, z + 1, c), device(x, y, z + 3, c)

    load_left = pltpu.make_async_copy(left.at[0], sbuf, l_sem.at[0])
    load_right = pltpu.make_async_copy(right.at[0], wbuf, l_sem.at[1])

    barrier = pltpu.get_barrier_semaphore()
    greeted = [device(x + d, y, z, c) for d in (1, 2, 3)]
    greeted += [device(x, y + d, z, c) for d in (1, 2, 3)]
    greeted += [device(x, y + d, z, 1 - c) for d in (0, 1, 2, 3)]
    greeted += [above, below, pair_across]
    for target in greeted:
        pl.semaphore_signal(barrier, inc=1, device_id=target, device_id_type=pl.DeviceIdType.MESH)
    pl.semaphore_wait(barrier, len(greeted))

    def arrived(ref, sem):
        push(ref, ref, x_send.at[0, 0], sem, other_core).wait_recv()

    finals = []

    def start(copy, when=None):
        if when is None:
            copy.start()
        else:
            pl.when(when)(copy.start)
        finals.append((when, copy))

    def a_rows(slot, t):
        return abuf.at[pl.ds(pl.multiple_of(TOK * slot + CH * t, CH), CH), :]

    def x_slot(source):
        return jnp.where(home, 4 * y + 2 * source + c, 16 + source)

    own_slot = x_slot(x_hi)
    for t in (LAST, 0, 1, 2):
        src = act.at[pl.ds(CH * t, CH), :]
        for n in range(2):
            target = 2 * x_lo + n
            start(
                push(src, a_rows(own_slot, t), x_send.at[n, t], x_recv.at[x_hi, t], device(target, y, z, c)),
                target != x,
            )
        stays = pltpu.make_async_copy(src, a_rows(own_slot, t), x_recv.at[x_hi, t])
        pl.when(x_lo == x_hi)(stays.start)

    g_own, g_far = 2 * x_hi + c, 2 * (1 - x_hi) + c

    def g_part(g, h, j):
        return gbuf.at[g, h, pl.ds(CH * j, CH), :]

    def g_sem(g, h, j):
        return g_recv.at[(2 * g + h) * GC + j]

    def cot_own(n, target, j):
        start(push(cot.at[pl.ds(CH * j, CH), :], g_part(g_own, p, j), g_send.at[n, j], g_sem(g_own, p, j), target))

    for j in range(GC):
        cot_own(2, pair, j)
        cot_own(0, across, j)
    for j in range(GC):
        cot_own(1, other_core, j)
    keep_g = pltpu.make_async_copy(cot, gbuf.at[g_own, p], lg_sem)
    keep_g.start()
    load_left.start()
    load_right.start()

    def t_rows(zs, source):
        final = TOK * (4 * y + 2 * source + c) + CH * LAST
        waits = jnp.where(zs == z, TOK * (16 + source) + CH * LAST, TOK * 18 + CH * (2 * zs + source))
        return abuf.at[pl.ds(pl.multiple_of(jnp.where(zs == mine_z, final, waits), CH), CH), :]

    def t_land(zs, source):
        final = TOK * (4 * y + 2 * source + c) + CH * LAST
        waits = TOK * 18 + CH * (2 * zs + source)
        return abuf.at[pl.ds(pl.multiple_of(jnp.where(zs == mine_z, final, waits), CH), CH), :]

    sources = [(x_hi + s) % 2 for s in range(2)]
    for s, source in enumerate(sources):
        arrived(a_rows(x_slot(source), LAST), x_recv.at[source, LAST])
        ref = t_rows(z, source)
        start(push(ref, t_land(z, source), z_send.at[0, s], z_recv.at[2 * z + source], above))
        start(push(ref, t_land(z, source), z_send.at[1, s], z_recv.at[2 * z + source], below))

    def along_y(t):
        for s, source in enumerate(sources):
            slot = x_slot(source)
            arrived(a_rows(slot, t), x_recv.at[source, t])
            for _, copy in z_copies(4 * t + 2 * s + c):
                pl.when(home)(copy.start)
            final = 4 * y + 2 * source + c
            for n, (when, dy) in enumerate(((odd == 1, 1), (odd == 1, 3), (odd == 0, 2))):
                start(
                    push(
                        a_rows(slot, t), a_rows(final, t), y_send.at[n, s, t], a_recv.at[final * 3 + t],
                        device(x, y + dy, z, k_home),
                    ),
                    when,
                )
            start(
                push(a_rows(slot, t), a_rows(final, t), y_send.at[3, s, t], a_recv.at[final * 3 + t], other_core),
                jnp.logical_and(odd == 0, c != k_home),
            )

    def source_y(q):
        return (y + q + (q // 2) * (1 - 2 * (q % 2))) % 4

    def step_of(step):
        own = step < 3
        rest = jnp.maximum(step - 3, 0)
        return jnp.where(own, step, rest // 3), jnp.where(own, 0, 1 + rest % 3)

    def order(i):
        t, q = step_of(i // 4)
        g = 2 * ((x_hi + (i % 4) // 2) % 2) + i % 2
        return t, q, 4 * source_y(q) + g

    def z_copies(i):
        t, _, slot = order(i)
        ref, number = a_rows(slot, t), slot * 3 + t
        up = push(ref, ref, up_send.at[number], a_recv.at[number], above)
        down = push(ref, ref, down_send.at[number], a_recv.at[number], below)
        go_up = jnp.logical_or(home, jnp.logical_and(rel == 3, i % 2 == 0))
        go_down = jnp.logical_or(home, jnp.logical_and(rel == 1, i % 2 == 1))
        return (go_up, up), (go_down, down)

    def relay(i, carry=0):
        t, q, slot = order(i)
        held = jnp.logical_and(home, jnp.logical_and(q == 0, i % 2 == c))

        @pl.when(jnp.logical_not(held))
        def _():
            arrived(a_rows(slot, t), a_recv.at[slot * 3 + t])
            for when, copy in z_copies(i):
                pl.when(when)(copy.start)

        return carry

    def relay_step(s):
        lax.fori_loop(4 * s, 4 * s + 4, relay, 0)

    def last_along_z():
        for s, (zs, source, target) in enumerate((((z + 3) % 4, 0, above), ((z + 1) % 4, 1, below))):
            ref = t_rows(zs, source)
            arrived(ref, z_recv.at[2 * zs + source])
            start(push(ref, t_land(zs, source), z_send.at[2, s], z_recv.at[2 * zs + source], target))

    def last_along_y():
        for zs, source in (((z + 3) % 4, 1), ((z + 1) % 4, 0), ((z + 2) % 4, 0), ((z + 2) % 4, 1)):
            arrived(t_rows(zs, source), z_recv.at[2 * zs + source])
        for source in range(2):
            final = 4 * y + 2 * source + c
            land = a_rows(final, LAST)
            near, there = 2 * c + p, 2 * (1 - c) + p
            near_odd, there_odd = 2 * c + 1 - p, 2 * (1 - c) + 1 - p
            for n, (zs, target) in enumerate((
                (there, other_core),
                (near_odd, device(x, y + 1, z, c)), (near_odd, device(x, y + 3, z, c)),
                (there_odd, device(x, y + 1, z, 1 - c)), (there_odd, device(x, y + 3, z, 1 - c)),
                (near, device(x, y + 2, z, c)), (there, device(x, y + 2, z, 1 - c)),
            )):
                start(push(t_rows(zs, source), land, t_send.at[source, n], t_recv.at[final], target))

    gd_count = [0]

    def to_core(g, h, j):
        start(push(g_part(g, h, j), g_part(g, h, j), gd_send.at[gd_count[0]], g_sem(g, h, j), other_core))
        gd_count[0] += 1

    def cot_pair(j):
        arrived(g_part(g_own, 1 - p, j), g_sem(g_own, 1 - p, j))
        start(push(g_part(g_own, 1 - p, j), g_part(g_own, 1 - p, j), gf_send.at[j], g_sem(g_own, 1 - p, j), across))
        to_core(g_own, 1 - p, j)

    def cot_far(h, j):
        arrived(g_part(g_far, h, j), g_sem(g_far, h, j))
        to_core(g_far, h, j)

    def from_core(h):
        for g in range(2):
            for j in range(GC):
                arrived(g_part(2 * g + 1 - c, h, j), g_sem(2 * g + 1 - c, h, j))

    def split_roots(i, carry):
        part = pl.ds(pl.multiple_of(128 * i, 128), 128)
        l1[part, :], l2[part, :] = split(sbuf[part, :])
        r1[part, :], r2[part, :] = split(wbuf[part, :])
        return carry

    def multiply(t, q, h):
        ys = source_y(q)
        value = None
        for g in range(4):
            product = lax.dot_general(
                abuf[pl.ds(pl.multiple_of(TOK * (4 * ys + g) + CH * t, CH), CH), :],
                gbuf[g, h, pl.ds(pl.multiple_of(CH * t, CH), CH), :],
                (((0,), (0,)), ((), ())), preferred_element_type=F32,
            )
            value = product if value is None else value + product
        gacc[pl.ds(pl.multiple_of(FEAT * ys, FEAT), FEAT), pl.ds(pl.multiple_of(HALF * h, HALF), HALF)] += value

    def multiply_all(t, q):
        ys = source_y(q)
        values = [None, None]
        for g in range(4):
            turned = abuf[pl.ds(pl.multiple_of(TOK * (4 * ys + g) + CH * t, CH), CH), :].T
            for h in range(2):
                product = mm(turned, gbuf[g, h, pl.ds(pl.multiple_of(CH * t, CH), CH), :])
                values[h] = product if values[h] is None else values[h] + product
        for h in range(2):
            gacc[pl.ds(pl.multiple_of(FEAT * ys, FEAT), FEAT), pl.ds(HALF * h, HALF)] += values[h]

    def multiply_early(h):
        def body(i, carry):
            multiply(*step_of(i), h)
            return carry

        return body

    along_y(0)
    along_y(1)
    along_y(2)
    last_along_z()
    last_along_y()
    relay_step(0)
    relay_step(1)
    cot_far(p, 0)
    cot_pair(0)
    load_left.wait()
    load_right.wait()
    lax.fori_loop(0, 8, split_roots, 0)
    relay_step(2)
    cot_far(p, 1)
    cot_pair(1)
    cot_far(p, 2)
    sbuf[...] = jnp.zeros_like(sbuf)
    gacc[...] = jnp.zeros_like(gacc)
    gsq[...] = jnp.zeros_like(gsq)
    ssq[...] = jnp.zeros_like(ssq)
    relay_step(3)
    cot_far(p, 3)
    relay_step(4)
    cot_pair(2)
    cot_far(1 - p, 0)
    relay_step(5)
    cot_pair(3)
    cot_far(1 - p, 1)
    from_core(p)
    keep_g.wait()
    relay_step(6)
    cot_far(1 - p, 2)
    lax.fori_loop(0, 4, multiply_early(p), 0)
    relay_step(7)
    cot_far(1 - p, 3)
    lax.fori_loop(4, 8, multiply_early(p), 0)
    relay_step(8)
    lax.fori_loop(8, 9, multiply_early(p), 0)
    from_core(1 - p)

    def last_steps(u, carry):
        @pl.when(u < 12)
        def _():
            relay(36 + u)

        lax.fori_loop(jnp.minimum(3 * u, 9), jnp.minimum(3 * u + 3, 9), multiply_early(1 - p), 0)
        q = (u + 1) // 3 - 1
        done = jnp.logical_or(jnp.logical_or(u == 3, u == 5), jnp.logical_or(u == 8, u == 12))

        @pl.when(done)
        def _():
            ys = source_y(q)
            for g in range(4):
                @pl.when(jnp.logical_not(jnp.logical_and(q == 0, c == g % 2)))
                def _():
                    arrived(a_rows(4 * ys + g, LAST), t_recv.at[4 * ys + g])

            def body(i, inner):
                multiply_all(2 + i, q)
                return inner

            lax.fori_loop(jnp.where(q == 0, 1, 0), 2, body, 0)

        at = jnp.logical_or(jnp.logical_or(u == 4, u == 6), jnp.logical_or(u == 9, u == 12))
        @pl.when(at)
        def _():
            q2 = u // 3 - 1
            ys = source_y(q2)
            columns = pl.ds(pl.multiple_of(FEAT * ys, FEAT), FEAT)
            value = gacc[columns, :]
            gsq[...] += jnp.sum(value * value, axis=0, keepdims=True)
            g1[...], g2[...] = split(value)

            def left_rows(r, inner):
                part = pl.ds(pl.multiple_of(256 * r, 256), 256)
                high = l1[part, columns]
                sbuf[part, :] += mm(high, g1[...]) + mm(high, g2[...]) + mm(l2[part, columns], g1[...])
                return inner

            lax.fori_loop(0, 4, left_rows, 0)

        return carry

    lax.fori_loop(0, 13, last_steps, 0)

    def right_rows(r, carry):
        part = pl.ds(pl.multiple_of(256 * r, 256), 256)
        high, low = split(sbuf[part, :])
        for h in range(2):
            cols = pl.ds(HALF * h, HALF)
            value = mm(high, r1[:, cols]) + mm(high, r2[:, cols]) + mm(low, r1[:, cols])
            wbuf[part, cols] = value
            ssq[:, cols] += jnp.sum(value * value, axis=0, keepdims=True)
        return carry

    lax.fori_loop(0, 4, right_rows, 0)
    count = BLK * BLK
    graft = jnp.sqrt(jnp.sum(gsq[...], axis=1, keepdims=True) / count + epsilon) / jnp.sqrt(
        jnp.sum(ssq[...], axis=1, keepdims=True) / count + epsilon
    )

    block = 4 * x_hi + 2 * c + p
    orows = BLK // OC

    def o_part(number, j):
        return out.at[pl.ds(pl.multiple_of(BLK * number + orows * j, orows), orows), :]

    def o_sem(number, j):
        return o_recv.at[number * OC + j]

    for j in range(OC + 1):
        if j < OC:
            for h in range(2):
                fin[h, pl.ds(orows * j, orows), :] = (
                    wbuf[pl.ds(orows * j, orows), pl.ds(HALF * h, HALF)] * graft
                ).astype(BF16)
        if j > 0:
            i = j - 1
            mine = fin.at[p, pl.ds(orows * i, orows), :]
            theirs = fin.at[1 - p, pl.ds(orows * i, orows), :]
            for n, (src, target) in enumerate(
                ((mine, across), (theirs, pair_across), (theirs, pair), (mine, other_core))
            ):
                start(push(src, o_part(block, i), o_send.at[n, i], o_sem(block, i), target))
            copy = pltpu.make_async_copy(mine, o_part(block, i), lo_sem.at[i])
            copy.start()
    p_core = 2 * c
    far = 4 * (1 - x_hi)
    for j in range(OC):
        for n, number in enumerate((4 * x_hi + p_core + 1 - p, far + p_core + p, far + p_core + 1 - p)):
            arrived(o_part(number, j), o_sem(number, j))
            start(push(o_part(number, j), o_part(number, j), od_send.at[n, j], o_sem(number, j), other_core))

    for j in range(OC):
        for number in (0, 1, 4, 5):
            arrived(o_part(number + 2 * (1 - c), j), o_sem(number + 2 * (1 - c), j))
        pltpu.make_async_copy(fin.at[p, pl.ds(orows * j, orows), :], o_part(block, j), lo_sem.at[j]).wait()
    for when, copy in finals:
        if when is None:
            copy.wait_send()
        else:
            pl.when(when)(copy.wait_send)

    def drain(i, carry):
        for when, copy in z_copies(i):
            pl.when(when)(copy.wait_send)
        return carry

    lax.fori_loop(0, 48, drain, 0)


def local(act, cot, left, right):
    dma = pltpu.SemaphoreType.DMA
    anywhere = pl.BlockSpec(memory_space=pl.ANY)
    return pl.pallas_call(
        kernel,
        out_shape=pltpu.VMEM((8 * BLK, HALF), BF16),
        in_specs=[anywhere] * 4,
        out_specs=anywhere,
        scratch_shapes=[
            pltpu.VMEM((20 * TOK, FEAT), BF16),
            pltpu.VMEM((4, 2, TOK, HALF), BF16),
            pltpu.VMEM((BLK, BLK), BF16), pltpu.VMEM((BLK, BLK), BF16),
            pltpu.VMEM((BLK, BLK), BF16), pltpu.VMEM((BLK, BLK), BF16),
            pltpu.VMEM((BLK, BLK), F32), pltpu.VMEM((BLK, BLK), F32),
            pltpu.VMEM((BLK, BLK), F32),
            pltpu.VMEM((FEAT, BLK), BF16), pltpu.VMEM((FEAT, BLK), BF16),
            pltpu.VMEM((1, BLK), F32), pltpu.VMEM((1, BLK), F32),
            pltpu.VMEM((2, BLK, HALF), BF16),
            dma((2, 4)), dma((2, 4)), dma((4, 2, 3)), dma((48,)), dma((48,)), dma((48,)),
            dma((8,)), dma((3, 2)), dma((16,)), dma((2, 7)),
            dma((8 * GC,)), dma((3, GC)), dma((GC,)), dma((3 * GC,)),
            dma((8 * OC,)), dma((4, OC)), dma((3, OC)), dma((2,)), dma, dma((OC,)),
        ],
        compiler_params=pltpu.CompilerParams(
            collective_id=0, has_side_effects=True, vmem_limit_bytes=46 * 1024 * 1024
        ),
        name="shampoo",
    )(act, cot, left, right)


def solution(mesh):
    in_specs = (P("gx", "gy"), P("gx", "gy"), P(("gx", "gy"), None, None), P(("gx", "gy"), None, None))
    return jax.shard_map(local, mesh=mesh, in_specs=in_specs, out_specs=P(None, "gy"), check_vma=False)
```
